32 devices in a mesh: gx: 2 (over x), gy: 4 (over z), ta: 4 (over y, core).
Axes of the slice: x: 2, y: 2, z: 4, core: 2. Of those that a mesh axis runs over, the one named last changes fastest.
Arguments:
- traces: bfloat16 [131072, 1024], P(('gx', 'gy'), 'ta'), may hold values from -6 to 6
- interp: bfloat16 [2, 16], replicated, may hold values from -1.5 to 1.5
- translations: bfloat16 [4, 2048, 1024], P(None, ('gx', 'gy')), may hold values from -0.125 to 0.125
- leaf_slot: int32 [8192], P(('gx', 'gy', 'ta')), may hold values from 0 to 255, as said below
- pairing: int32 [4, 8192], P(None, ('gx', 'gy', 'ta')), may hold values from 0 to 255, as said below
Outputs:
- coefficients: bfloat16 [8192, 1024], P(('gx', 'gy', 'ta'))
The draws below stay inside these ranges and needn't reach their ends.
Inputs may be any that keep to these rules, and one draw needn't show every extreme that they name: `leaf_slot`: each aligned block of 256 entries (the leaves of one device) is a permutation of 0 to 255. `pairing`: for every level, each aligned block of 256 entries along the leaves is a permutation of 0 to 255.
All inputs are finite; a program needn't handle non-finite values.
Results may differ from the reference program's by a relative error of at most 0.0082.
Values may be sent and summed in bfloat16 or wider, within the bound.
A program may use at most 128 MiB of HBM per device.

```python
import math
import jax
import jax.numpy as jnp
from jax import lax

NT = 1024
NF = 256
CHEB = 2
BOXT = 16
LEVELS = 4
BOX_DEV = 256
W = 1024
NBOX = 8192
NTRACE = 131072
N_GX = 2
N_GY = 4
N_TA = 4


def block_perms(key, blocks, width):
    keys = jax.random.split(key, blocks)
    return jax.vmap(lambda subkey: jax.random.permutation(subkey, width))(keys).astype(jnp.int32)


def draw_leaf_slot(key, part):
    return block_perms(jax.random.fold_in(key, 11), NBOX // BOX_DEV, BOX_DEV).reshape(NBOX)


def draw_pairing(key, part):
    return block_perms(jax.random.fold_in(key, 23), LEVELS * (NBOX // BOX_DEV), BOX_DEV).reshape(LEVELS, NBOX)


def levels(key, shape, cuts, least, largest):
    loudness = 1.0
    for dim, parts in cuts:
        draws = jax.random.uniform(jax.random.fold_in(jax.random.fold_in(key, 6), dim), (parts,), jnp.float32, least / len(cuts), largest / len(cuts))
        loudness = loudness * jnp.repeat(jnp.exp(draws), shape[dim] // parts).reshape((-1,) + (1,) * (len(shape) - 1 - dim))
    return loudness


def scatter_about(key, extent, scale, limit, pieces=(), kind=jnp.bfloat16):
    level = levels(key, extent, pieces, -0.22, 0.18) if pieces else 1.0
    values = jax.random.normal(key, extent, jnp.float32) * scale * level
    return jnp.minimum(jnp.maximum(values, -limit), limit).astype(kind)


def setup_inputs(seed: int = 0) -> dict:
    splits = jax.random.split(jax.random.key(seed), 6)
    return {
        "traces": scatter_about(splits[0], (NTRACE, NT), 1.0, 6.0, ((0, 8), (1, 4))),
        "interp": scatter_about(splits[1], (CHEB, BOXT), BOXT ** -0.5, 1.5),
        "translations": scatter_about(splits[2], (LEVELS, 2 * W, W), (2 * W) ** -0.5, 0.125, ((1, 8),)),
        "leaf_slot": draw_leaf_slot(jax.random.fold_in(splits[5], 71), 0),
        "pairing": draw_pairing(jax.random.fold_in(splits[5], 71), 0),
    }


def spectrum_table(length, count):
    sample_pos = lax.broadcasted_iota(jnp.float32, (length, count), 0)
    frequency = lax.broadcasted_iota(jnp.float32, (length, count), 1) + 1.0
    angles = 2.0 * math.pi / length * jnp.mod(sample_pos * frequency, float(length))
    factor = math.sqrt(2.0 / length)
    return jnp.concatenate([jnp.cos(angles) * factor, -jnp.sin(angles) * factor], axis=1).astype(jnp.bfloat16)

def reference(traces, interp, translations, leaf_slot, pairing):
    devices = N_GX * N_GY * N_TA
    groups = N_GX * N_GY
    per_peer = BOX_DEV // groups
    fourier = spectrum_table(NT, NF)
    weights = interp.astype(jnp.float32)

    def one_device(device_block):
        sampled = jnp.einsum('cb,kbt->kct', weights, device_block.astype(jnp.float32), precision=lax.Precision.HIGHEST)
        sampled = sampled.astype(jnp.bfloat16).reshape(BOX_DEV * CHEB, NT)
        spectra = jnp.dot(sampled, fourier, preferred_element_type=jnp.float32)
        return spectra.reshape(BOX_DEV, CHEB * 2 * NF).astype(jnp.bfloat16)
    cheb_points = lax.map(one_device, traces.reshape(devices, BOX_DEV, BOXT, NT))
    cheb_points = cheb_points.reshape(NBOX, CHEB * 2 * NF)
    leaves = jnp.arange(NBOX, dtype=jnp.int32)
    owners = leaves // BOX_DEV
    group_index = owners // N_TA
    ta_index = owners % N_TA
    source_group = leaf_slot // per_peer
    offset = leaf_slot % per_peer
    source_rows = ((source_group * N_TA + ta_index) * BOX_DEV + group_index * per_peer + offset).astype(jnp.int32)
    states = cheb_points[source_rows]
    log_devices = devices.bit_length() - 1
    for layer_index in range(LEVELS):
        flip_bit = layer_index * log_devices // LEVELS
        partner = ((owners ^ 1 << flip_bit) * BOX_DEV + pairing[layer_index]).astype(jnp.int32)
        joined = jnp.concatenate([states, states[partner]], axis=1).astype(jnp.float32)
        product_sum = jnp.dot(joined, translations[layer_index].astype(jnp.float32), precision=lax.Precision.HIGHEST)
        states = product_sum.astype(jnp.bfloat16)
    return states
```

```python
import functools
import math

import jax
import jax.numpy as jnp
import numpy as np
from jax import lax
from jax.experimental import pallas as pl
from jax.experimental.pallas import tpu as pltpu
from jax.sharding import PartitionSpec as P

NF = 256
CHEB = 2
BOXT = 16
BLOCK_BOXES = 16
TILE = 256
MESH = pl.DeviceIdType.MESH


def spectrum_table(length, count):
    sample_pos = np.arange(length, dtype=np.float32)[:, None]
    frequency = np.arange(count, dtype=np.float32)[None, :] + np.float32(1.0)
    angles = np.float32(2.0 * math.pi / length) * np.mod(sample_pos * frequency, np.float32(length))
    factor = np.float32(math.sqrt(2.0 / length))
    table = np.concatenate([np.cos(angles) * factor, -np.sin(angles) * factor], axis=1)
    return table.astype(jnp.bfloat16)


def flip(index, mask, size):
    result = index
    bit = 1
    while bit < size:
        if mask & bit:
            result = result + bit - 2 * bit * ((index // bit) % 2)
        bit *= 2
    return result


def kernel(
    sizes,
    traces,
    interp,
    translations,
    slots,
    pairs,
    table,
    out,
    tr,
    weights,
    mat,
    sampled,
    slices,
    fourier,
    acc,
    points,
    arrived,
    states,
    partner,
    select,
    load_sem,
    table_sem,
    own_sem,
    ag_send,
    ag_recv,
    core_send,
    core_recv,
    ta_send,
    ta_recv,
    g_send,
    g_recv,
    level_send,
    level_recv,
):
    n_gx, n_gy, n_ta = sizes
    groups = n_gx * n_gy
    gx, gy, ta = lax.axis_index("gx"), lax.axis_index("gy"), lax.axis_index("ta")
    group = gx * n_gy + gy
    level_count = translations.shape[0]
    rows = translations.shape[1]
    half = rows // 2
    width = translations.shape[2]
    boxes = slots.shape[1]
    span = traces.shape[1]
    block = boxes * BOXT
    chunk = states.shape[3]
    chunks = width // chunk
    log_devices = (groups * n_ta).bit_length() - 1
    side = ta % 2

    def of_group(offset):
        p = flip(group, offset, groups)
        return (p // n_gy, p % n_gy, ta)

    def of_ta(offset):
        return (gx, gy, flip(ta, offset, n_ta))

    def loading(j):
        t = flip(ta, j, n_ta)
        return pltpu.make_async_copy(
            traces.at[pl.ds(pl.multiple_of(t * block, block), block), :], tr.at[j], load_sem.at[j]
        )

    def own(level):
        return [
            pltpu.make_async_copy(
                translations.at[level, pl.ds(part * half, half), :],
                weights.at[level, group, part],
                own_sem.at[level, part],
            )
            for part in range(2)
        ]

    bits = []
    bit = n_gy // 2
    while bit:
        bits.append(bit)
        bit //= 2
    bit = n_gx // 2
    while bit:
        bits.append(bit * n_gy)
        bit //= 2
    stage_of = {0: -1}
    order = [0]
    for stage, bit in enumerate(bits):
        for offset in list(order):
            stage_of[offset ^ bit] = stage
            order.append(offset ^ bit)

    def shard(level, offset):
        return weights.at[level, flip(group, offset, groups), side]

    def passing(level, offset, stage):
        bit = bits[stage]
        return pltpu.make_async_remote_copy(
            src_ref=shard(level, offset),
            dst_ref=shard(level, offset),
            send_sem=ag_send.at[level, offset ^ bit],
            recv_sem=ag_recv.at[level, offset ^ bit],
            device_id=of_group(bit),
            device_id_type=MESH,
        )

    def landed(level, offset):
        bit = bits[stage_of[offset]]
        return pltpu.make_async_remote_copy(
            src_ref=shard(level, offset),
            dst_ref=shard(level, offset),
            send_sem=ag_send.at[level, offset],
            recv_sem=ag_recv.at[level, offset],
            device_id=of_group(bit),
            device_id_type=MESH,
        )

    def sharing(level, offset, mine):
        place = weights.at[
            level, flip(group, offset, groups), side if mine else flip(side, 1, 2)
        ]
        return pltpu.make_async_remote_copy(
            src_ref=place,
            dst_ref=place,
            send_sem=core_send.at[level, offset],
            recv_sem=core_recv.at[level, offset],
            device_id=of_ta(1),
            device_id_type=MESH,
        )

    def pump(level, stage):
        if stage == 0:
            for copy in own(level):
                copy.wait()
        for offset in order:
            if stage_of[offset] != stage - 1:
                continue
            if offset:
                landed(level, offset).wait_recv()
                sharing(level, offset, True).start()
            for later in range(stage, len(bits)):
                passing(level, offset, later).start()

    stages = len(bits)

    reached = [0]

    def pumps(step):
        while reached[0] <= step:
            for level in range(level_count):
                stage = reached[0] - level
                if 0 <= stage <= stages:
                    pump(level, stage)
            reached[0] += 1

    def finish(level):
        for offset in order[1:]:
            sharing(level, offset, False).wait_recv()

    def regroup(j):
        return pltpu.make_async_remote_copy(
            src_ref=sampled.at[j],
            dst_ref=slices.at[j],
            send_sem=ta_send.at[j],
            recv_sem=ta_recv.at[j],
            device_id=of_ta(j),
            device_id_type=MESH,
        )

    def moving(offset, sending):
        src = points.at[flip(group, offset, groups)]
        dst = arrived.at[group if sending else flip(group, offset, groups)]
        return pltpu.make_async_remote_copy(
            src_ref=src,
            dst_ref=dst,
            send_sem=g_send.at[offset],
            recv_sem=g_recv.at[offset],
            device_id=of_group(offset),
            device_id_type=MESH,
        )

    def exchange(level, k):
        mask = 2 ** (level * log_devices // level_count)
        target = of_ta(mask) if mask < n_ta else of_group(mask // n_ta)
        return pltpu.make_async_remote_copy(
            src_ref=states.at[level, k],
            dst_ref=partner.at[level, k],
            send_sem=level_send.at[level, k],
            recv_sem=level_recv.at[level, k],
            device_id=target,
            device_id_type=MESH,
        )

    near = [n_ta - 1 - j for j in range(n_ta)]
    for j in near:
        loading(j).start()
    for level in range(level_count):
        for copy in own(level):
            copy.start()
    table_copy = pltpu.make_async_copy(table, fourier, table_sem)
    table_copy.start()

    barrier = pltpu.get_barrier_semaphore()
    for j in range(1, n_ta):
        pl.semaphore_signal(barrier, inc=1, device_id=of_ta(j), device_id_type=MESH)
    for offset in range(1, groups):
        pl.semaphore_signal(barrier, inc=1, device_id=of_group(offset), device_id_type=MESH)

    columns = BLOCK_BOXES * BOXT
    spread = (
        lax.broadcasted_iota(jnp.int32, (BOXT, columns), 1) % BOXT
        == lax.broadcasted_iota(jnp.int32, (BOXT, columns), 0)
    )
    tiled = jnp.dot(
        interp[...], spread.astype(jnp.float32).astype(jnp.bfloat16), preferred_element_type=jnp.float32
    )
    own_box = (
        lax.broadcasted_iota(jnp.int32, (BLOCK_BOXES, columns), 1) // BOXT
        == lax.broadcasted_iota(jnp.int32, (BLOCK_BOXES, columns), 0)
    )
    for c in range(CHEB):
        mat[pl.ds(c * BLOCK_BOXES, BLOCK_BOXES), :] = jnp.where(
            own_box, tiled[c : c + 1, :], 0.0
        ).astype(jnp.bfloat16)

    def selection(index_row):
        hit = lax.broadcasted_iota(jnp.int32, (boxes, boxes), 0) == index_row
        return jnp.where(hit, 1.0, 0.0).T.astype(jnp.bfloat16)

    select[0] = selection(slots[...])
    for level in range(level_count):
        select[level + 1] = selection(pairs[pl.ds(level, 1), :])

    pl.semaphore_wait(barrier, n_ta - 1 + groups - 1)
    pumps(0)

    for j in near:
        loading(j).wait()
        where = sampled if j else slices

        def interpolate(i, carry):
            traces_block = tr[j, pl.ds(pl.multiple_of(i * columns, columns), columns), :]
            both = jnp.dot(mat[...], traces_block, preferred_element_type=jnp.float32)
            both = both.astype(jnp.bfloat16)
            place = pl.ds(pl.multiple_of(i * BLOCK_BOXES, BLOCK_BOXES), BLOCK_BOXES)
            for c in range(CHEB):
                where[j, c, place, :] = both[c * BLOCK_BOXES : (c + 1) * BLOCK_BOXES, :]
            return carry

        lax.fori_loop(0, boxes // BLOCK_BOXES, interpolate, 0, unroll=4)
        if j:
            regroup(j).start()

    pumps(1)
    table_copy.wait()
    for j in range(n_ta):
        if j:
            regroup(j).wait_recv()
        first = pl.multiple_of(flip(ta, j, n_ta) * span, span)
        for c in range(CHEB):
            part = jnp.dot(
                slices[j, c], fourier[pl.ds(first, span), :], preferred_element_type=jnp.float32
            )
            cols = pl.ds(c * 2 * NF, 2 * NF)
            if j:
                acc[:, cols] += part
            else:
                acc[:, cols] = part
    points[...] = acc[...].reshape(points.shape).astype(jnp.bfloat16)
    for offset in range(groups - 1, 0, -1):
        moving(offset, True).start()
    arrived[group] = points[group]
    pumps(2)
    for offset in range(1, groups):
        moving(offset, False).wait_recv()

    for k in range(chunks):
        boxes_in = arrived[:, :, k * chunk : (k + 1) * chunk].astype(jnp.float32)
        boxes_in = boxes_in.reshape(boxes, chunk).astype(jnp.bfloat16)
        states[0, k] = jnp.dot(select[0], boxes_in, preferred_element_type=jnp.float32).astype(
            jnp.bfloat16
        )
        exchange(0, k).start()

    per_chunk = chunk // rows

    def weight(level, k, cols):
        piece = weights[level, k * per_chunk : (k + 1) * per_chunk, :, :, cols]
        return piece.reshape(chunk, chunk)

    for level in range(level_count):
        pumps(level + stages)
        finish(level)

        def own_part(n, carry):
            cols = pl.ds(pl.multiple_of(n * chunk, chunk), chunk)
            total = jnp.zeros((boxes, chunk), jnp.float32)
            for k in range(chunks):
                total += jnp.dot(
                    states[level, k], weight(level, k, cols), preferred_element_type=jnp.float32
                )
            acc[:, cols] = total
            return carry

        lax.fori_loop(0, chunks, own_part, 0)
        for k in range(chunks):
            exchange(level, k).wait_recv()
            aligned = jnp.dot(
                select[level + 1], partner[level, k], preferred_element_type=jnp.float32
            ).astype(jnp.bfloat16)
            if k < chunks - 1:

                def partner_part(n, carry):
                    cols = pl.ds(pl.multiple_of(n * chunk, chunk), chunk)
                    acc[:, cols] += jnp.dot(
                        aligned, weight(level, chunks + k, cols), preferred_element_type=jnp.float32
                    )
                    return carry

                lax.fori_loop(0, chunks, partner_part, 0)
            else:
                for n in range(chunks):
                    cols = pl.ds(n * chunk, chunk)
                    total = acc[:, cols] + jnp.dot(
                        aligned, weight(level, chunks + k, cols), preferred_element_type=jnp.float32
                    )
                    if level < level_count - 1:
                        states[level + 1, n] = total.astype(jnp.bfloat16)
                        exchange(level + 1, n).start()
                    else:
                        out[:, cols] = total.astype(jnp.bfloat16)

    for j in range(1, n_ta):
        regroup(j).wait_send()
    for offset in range(1, groups):
        moving(offset, True).wait_send()
    for level in range(level_count):
        for k in range(chunks):
            exchange(level, k).wait_send()
        for offset in order[1:]:
            landed(level, offset).wait_send()
            sharing(level, offset, True).wait_send()


def on_device(sizes, traces, interp, translations, leaf_slot, pairing):
    n_gx, n_gy, n_ta = sizes
    groups = n_gx * n_gy
    boxes = leaf_slot.shape[0]
    levels, rows, width = translations.shape
    span = traces.shape[1]
    block = traces.shape[0] // n_ta
    chunk = max(TILE, rows)
    chunks = width // chunk
    table = jnp.asarray(spectrum_table(span * n_ta, NF))
    bf16, f32 = jnp.bfloat16, jnp.float32
    anywhere = pl.BlockSpec(memory_space=pl.ANY)
    vmem = pl.BlockSpec(memory_space=pltpu.VMEM)
    dma = pltpu.SemaphoreType.DMA
    return pl.pallas_call(
        functools.partial(kernel, sizes),
        out_shape=jax.ShapeDtypeStruct((boxes, width), bf16),
        in_specs=[anywhere, vmem, anywhere, vmem, vmem, anywhere],
        out_specs=vmem,
        scratch_shapes=[
            pltpu.VMEM((n_ta, block, span), bf16),
            pltpu.VMEM((levels, groups, 2, rows // 2, width), bf16),
            pltpu.VMEM((CHEB * BLOCK_BOXES, BLOCK_BOXES * BOXT), bf16),
            pltpu.VMEM((n_ta, CHEB, boxes, span), bf16),
            pltpu.VMEM((n_ta, CHEB, boxes, span), bf16),
            pltpu.VMEM(table.shape, bf16),
            pltpu.VMEM((boxes, width), f32),
            pltpu.VMEM((groups, boxes // groups, width), bf16),
            pltpu.VMEM((groups, boxes // groups, width), bf16),
            pltpu.VMEM((levels, chunks, boxes, chunk), bf16),
            pltpu.VMEM((levels, chunks, boxes, chunk), bf16),
            pltpu.VMEM((levels + 1, boxes, boxes), bf16),
            dma((n_ta,)),
            dma,
            dma((levels, 2)),
            dma((levels, groups)),
            dma((levels, groups)),
            dma((levels, groups)),
            dma((levels, groups)),
            dma((n_ta,)),
            dma((n_ta,)),
            dma((groups,)),
            dma((groups,)),
            dma((levels, chunks)),
            dma((levels, chunks)),
        ],
        compiler_params=pltpu.CompilerParams(
            collective_id=0, has_side_effects=True, vmem_limit_bytes=60 * 2**20
        ),
    )(traces, interp, translations, leaf_slot.reshape(1, boxes), pairing, table)


def solution(mesh):
    sizes = (mesh.shape["gx"], mesh.shape["gy"], mesh.shape["ta"])
    in_specs = (
        P(("gx", "gy"), "ta"),
        P(),
        P(None, ("gx", "gy"), None),
        P(("gx", "gy", "ta")),
        P(None, ("gx", "gy", "ta")),
    )
    out_specs = P(("gx", "gy", "ta"), None)
    return jax.shard_map(
        functools.partial(on_device, sizes),
        mesh=mesh,
        in_specs=in_specs,
        out_specs=out_specs,
        check_vma=False,
    )
```
